32 devices in a mesh: seq: 16 (over z, y, x), dp: 2 (over core).
Axes of the slice: x: 2, y: 2, z: 4, core: 2. Of those that a mesh axis runs over, the one named last changes fastest.
Arguments:
- queries: bfloat16 [2, 3072, 4096], P('dp', 'seq'), may hold values from -6 to 6
- key_vectors: bfloat16 [2, 3072, 4096], P('dp', 'seq'), may hold values from -0.52734375 to 0.52734375
- value_vectors: bfloat16 [2, 3072, 4096], P('dp', 'seq'), may hold values from -6 to 6
- out_grad: bfloat16 [2, 3072, 4096], P('dp', 'seq'), may hold values from -8 to 8
- log_decay: float32 [2, 32, 3072], P('dp', None, 'seq'), may hold values from -0.7729167 to 0, as said below
- norm_gain: float32 [4096], replicated, may hold values from 0.25 to 1.75
Outputs:
- output: bfloat16 [2, 3072, 4096], P('dp', 'seq')
- grad_queries: bfloat16 [2, 3072, 4096], P('dp', 'seq')
- grad_keys: bfloat16 [2, 3072, 4096], P('dp', 'seq')
- grad_values: bfloat16 [2, 3072, 4096], P('dp', 'seq')
- grad_gain: float32 [4096], P('seq')
The draws below stay inside these ranges and needn't reach their ends.
Inputs may be any that keep to these rules, and one draw needn't show every extreme that they name: `log_decay`: every entry is negative.
All inputs are finite; a program needn't handle non-finite values.
Results may differ from the reference program's by a relative error of at most 0.006.
Values may be sent and summed in bfloat16 or wider, within the bound.
A program may use at most 128 MiB of HBM per device.

```python
import math
import jax
import jax.numpy as jnp
from jax import lax

HEADS = 32
HEAD_DIM = 128
TOK_DEV = 192
SEQUENCE_LENGTH = 3072
SEQS = 2


def draw_log_decay(key, part):
    head_random_key, quick_random_key, gradual_random_key, noise_random_key, spike_random_key, dropout_random_key = jax.random.split(key, 6)
    chosen = jax.random.uniform(head_random_key, (HEADS,))
    is_fast = chosen < 0.5
    fast_rate = jnp.exp(jax.random.uniform(quick_random_key, (HEADS,), minval=math.log(4.0 / TOK_DEV), maxval=math.log(7.0 / TOK_DEV)))
    slow_rate = jnp.exp(jax.random.uniform(gradual_random_key, (HEADS,), minval=math.log(0.1 / SEQUENCE_LENGTH), maxval=math.log(0.5 / SEQUENCE_LENGTH)))
    baseline_decay_rate = jnp.where(is_fast, fast_rate, slow_rate)
    sharding_arrangement = (SEQS, HEADS, SEQUENCE_LENGTH)
    decay_noise = jnp.exp(jax.random.uniform(noise_random_key, sharding_arrangement, minval=-0.69, maxval=0.69))
    decay_spikes = jax.random.uniform(spike_random_key, sharding_arrangement) < 2.0 / SEQUENCE_LENGTH
    dropped_log_decay = jax.random.uniform(dropout_random_key, sharding_arrangement, minval=-0.69, maxval=-0.22)
    return (-baseline_decay_rate[None, :, None] * decay_noise + jnp.where(decay_spikes, dropped_log_decay, 0.0)).astype(jnp.float32)


def spiked(entries, own_key, source, target, parts, factor):
    def block_of(dim):
        return (jnp.arange(entries.shape[dim]) // (entries.shape[dim] // parts)).reshape((-1,) + (1,) * (entries.ndim - 1 - dim))

    near = jax.random.permutation(own_key, parts)[block_of(target)]
    other_side = (block_of(target) + parts // 2) % parts
    return jnp.where((block_of(source) == near) | (block_of(source) == other_side), factor * entries, entries)


def level_of(key, extent, shards, low, largest):
    factor_of, own = 1.0, jax.random.fold_in(key, 6)
    for position, shards_of in shards:
        heights = jnp.exp(jax.random.uniform(jax.random.fold_in(own, position), (shards_of,), jnp.float32, low / len(shards), largest / len(shards)))
        factor_of = factor_of * jnp.repeat(heights, extent[position] // shards_of).reshape([-1 if axis == position else 1 for axis in range(len(extent))])
    return factor_of


def noise(key, extent, deviation, bound, pieces=(), kind=jnp.bfloat16):
    gain = level_of(key, extent, pieces, -0.22, 0.18) if pieces else 1.0
    drawn = jax.random.normal(key, extent, jnp.float32) * deviation * gain
    return jnp.minimum(jnp.maximum(drawn, -bound), bound).astype(kind)


def heavy_noise(rng, dims, width, most, cuts, heavy, held_as=jnp.bfloat16):
    drawn = width * jax.random.normal(rng, dims, jnp.float32)
    if cuts:
        drawn = drawn * level_of(rng, dims, cuts, -0.22, 0.18)
    return jnp.clip(spiked(drawn, jax.random.fold_in(rng, 3), *heavy), -most, most).astype(held_as)


def setup_inputs(seed: int = 0) -> dict:
    splits = jax.random.split(jax.random.key(seed), 7)
    queries = noise(splits[0], (SEQS, SEQUENCE_LENGTH, HEADS * HEAD_DIM), 1.0, 6.0, ((0, 2), (1, 16)))
    key_vectors = noise(splits[1], (SEQS, SEQUENCE_LENGTH, HEADS * HEAD_DIM), (HEAD_DIM ** -0.5), 0.52734375, ((0, 2), (1, 16)))
    value_vectors = noise(splits[2], (SEQS, SEQUENCE_LENGTH, HEADS * HEAD_DIM), 1.0, 6.0, ((0, 2), (1, 16)))
    out_grad = heavy_noise(splits[3], (SEQS, SEQUENCE_LENGTH, HEADS * HEAD_DIM), 1.0, 8.0, ((0, 2), (1, 16)), (1, 2, 16, 2.0))
    log_decay = draw_log_decay(jax.random.fold_in(splits[6], 71), 0)
    norm_gain = jnp.clip(1.0 + 0.15 * jax.random.normal(splits[5], (HEADS * HEAD_DIM,), jnp.float32), 0.25, 1.75)
    return {"queries": queries, "key_vectors": key_vectors, "value_vectors": value_vectors, "out_grad": out_grad, "log_decay": log_decay, "norm_gain": norm_gain}


epsilon = 1e-06

def widen(array):
    return array.astype(jnp.float32)

def decays(cumul, block_total, block_len):
    positions = jnp.arange(block_len)
    causal = (positions[:, None] >= positions[None, :])[None]
    log_gap = cumul[:, :, None] - cumul[:, None, :]
    weight = jnp.where(causal, jnp.exp(jnp.where(causal, log_gap, 0.0)), 0.0)
    start_scale = jnp.exp(cumul).T[:, :, None]
    end_scale = jnp.exp(block_total[:, None] - cumul).T[:, :, None]
    return (weight, start_scale, end_scale)

def single_sequence(inputs):
    query_seq, key_seq, value_seq, grad_seq, decay_seq, norm_gain = inputs
    length, feature_count = query_seq.shape
    head_count = decay_seq.shape[0]
    head_size = feature_count // head_count
    block_len = TOK_DEV
    block_count = length // block_len
    sequence_partition = (block_count, block_len, head_count, head_size)
    query_blocks = query_seq.reshape(sequence_partition)
    key_blocks = key_seq.reshape(sequence_partition)
    value_blocks = value_seq.reshape(sequence_partition)
    decay_blocks = decay_seq.reshape(head_count, block_count, block_len).transpose(1, 0, 2)
    cumulative = jnp.cumsum(decay_blocks, axis=2)
    totals = cumulative[:, :, -1]

    def forward_step(state, inputs_now):
        query_now, key_now, value_now, cumul, block_total = inputs_now
        weight, start_scale, end_scale = decays(cumul, block_total, block_len)
        scores = jnp.einsum('ihe,jhe->hij', widen(query_now), widen(key_now))
        weighted = (scores * weight).astype(jnp.bfloat16)
        inside = jnp.einsum('hij,jhe->ihe', widen(weighted), widen(value_now))
        prior_state = state.astype(jnp.bfloat16)
        carried = jnp.einsum('ihd,hde->ihe', widen(query_now), widen(prior_state)) * start_scale
        key_decayed = (widen(key_now) * end_scale).astype(jnp.bfloat16)
        local_state = jnp.einsum('jhd,jhe->hde', widen(key_decayed), widen(value_now))
        next_state = jnp.exp(block_total)[:, None, None] * state + local_state
        return (next_state, (inside + carried, prior_state))
    start = jnp.zeros((head_count, head_size, head_size), jnp.float32)
    unused, (attended, priors) = lax.scan(forward_step, start, (query_blocks, key_blocks, value_blocks, cumulative, totals))
    inv_rms = lax.rsqrt(lax.optimization_barrier(jnp.mean(attended * attended, axis=-1, keepdims=True)) + epsilon)
    normed = attended * inv_rms
    gain_heads = norm_gain.reshape(head_count, head_size)
    output = (normed * gain_heads).astype(jnp.bfloat16)
    grad_out = widen(grad_seq.reshape(sequence_partition))
    scaled = grad_out * gain_heads
    grad_attended = (inv_rms * (scaled - normed * lax.optimization_barrier(jnp.mean(scaled * normed, axis=-1, keepdims=True)))).astype(jnp.bfloat16)
    gain_term = lax.optimization_barrier(jnp.sum(grad_out * normed, axis=(0, 1))).reshape(feature_count)

    def backward_step(later, inputs_now):
        query_now, key_now, value_now, grad_now, cumul, block_total, prior_state = inputs_now
        weight, start_scale, end_scale = decays(cumul, block_total, block_len)
        scores = jnp.einsum('ihe,jhe->hij', widen(query_now), widen(key_now))
        weighted = (scores * weight).astype(jnp.bfloat16)
        later_state = later.astype(jnp.bfloat16)
        grad_scores = jnp.einsum('ihe,jhe->hij', widen(grad_now), widen(value_now))
        grad_weighted = (grad_scores * weight).astype(jnp.bfloat16)
        grad_query = jnp.einsum('hij,jhd->ihd', widen(grad_weighted), widen(key_now)) + start_scale * jnp.einsum('ihe,hde->ihd', widen(grad_now), widen(prior_state))
        grad_key = jnp.einsum('hij,ihd->jhd', widen(grad_weighted), widen(query_now)) + end_scale * jnp.einsum('jhe,hde->jhd', widen(value_now), widen(later_state))
        grad_value = jnp.einsum('hij,ihe->jhe', widen(weighted), widen(grad_now)) + end_scale * jnp.einsum('jhd,hde->jhe', widen(key_now), widen(later_state))
        query_decayed = (widen(query_now) * start_scale).astype(jnp.bfloat16)
        later_local = jnp.einsum('ihd,ihe->hde', widen(query_decayed), widen(grad_now))
        next_later = later_local + jnp.exp(block_total)[:, None, None] * later
        return (next_later, (grad_query.astype(jnp.bfloat16), grad_key.astype(jnp.bfloat16), grad_value.astype(jnp.bfloat16)))
    unused_later, grads = lax.scan(backward_step, start, (query_blocks, key_blocks, value_blocks, grad_attended, cumulative, totals, priors), reverse=True)
    shape_out = (length, feature_count)
    return (output.reshape(shape_out), grads[0].reshape(shape_out), grads[1].reshape(shape_out), grads[2].reshape(shape_out), gain_term)

def reference(queries, key_vectors, value_vectors, out_grad, log_decay, norm_gain):
    seq_count = queries.shape[0]
    gains = jnp.broadcast_to(norm_gain, (seq_count,) + norm_gain.shape)
    results = lax.map(single_sequence, (queries, key_vectors, value_vectors, out_grad, log_decay, gains))
    return (results[0], results[1], results[2], results[3], lax.optimization_barrier(jnp.sum(results[4], axis=0)))
```

```python
import functools

import jax
import jax.numpy as jnp
from jax import lax
from jax.experimental import pallas as pl
from jax.experimental.pallas import tpu as pltpu
from jax.sharding import PartitionSpec as P

epsilon = 1e-06
F32 = jnp.float32
BF16 = jnp.bfloat16
MESH = pl.DeviceIdType.MESH
NEG = -1e30


def dot_nn(a, b):
    return lax.dot_general(a, b, (((1,), (0,)), ((), ())), preferred_element_type=F32)


def dot_nt(a, b):
    return lax.dot_general(a, b, (((1,), (1,)), ((), ())), preferred_element_type=F32)


def dot_tn(a, b):
    return lax.dot_general(a, b, (((0,), (0,)), ((), ())), preferred_element_type=F32)


def cumulative(ld):
    tokens = ld.shape[1]
    i = lax.broadcasted_iota(jnp.int32, (tokens, tokens), 0)
    j = lax.broadcasted_iota(jnp.int32, (tokens, tokens), 1)
    lower = (i >= j).astype(F32)
    exact = lax.Precision.HIGHEST
    rows = lax.dot_general(
        ld, lower, (((1,), (1,)), ((), ())), precision=exact, preferred_element_type=F32
    )
    columns = lax.dot_general(
        lower, ld, (((1,), (1,)), ((), ())), precision=exact, preferred_element_type=F32
    )
    return rows, columns, i >= j


def local_kernel(heads, size, k_ref, v_ref, ld_ref, l_ref, a_ref):
    ld = ld_ref[0]
    rows, columns, _ = cumulative(ld)
    tokens = ld.shape[1]
    last = columns[tokens - 1 :, :]
    end = jnp.exp(last - columns)
    for h in range(heads):
        cols = slice(h * size, (h + 1) * size)
        kd = (k_ref[:, cols].astype(F32) * end[:, h : h + 1]).astype(BF16)
        l_ref[h] = dot_tn(kd, v_ref[:, cols]).astype(BF16)
        a_ref[0, h : h + 1, :] = jnp.broadcast_to(jnp.exp(last[:, h : h + 1]), (1, size))


def forward_kernel(
    heads, size, q_ref, k_ref, v_ref, g_ref, ld_ref, gain_ref, p_ref,
    out_ref, ga_ref, l_ref, term_ref,
):
    ld = ld_ref[0]
    rows, columns, causal = cumulative(ld)
    start = jnp.exp(columns)
    for h in range(heads):
        cols = slice(h * size, (h + 1) * size)
        q, k, v = q_ref[:, cols], k_ref[:, cols], v_ref[:, cols]
        weight = jnp.exp(jnp.where(causal, columns[:, h : h + 1] - rows[h : h + 1, :], NEG))
        weighted = (dot_nt(q, k) * weight).astype(BF16)
        begin = start[:, h : h + 1]
        attended = dot_nn(weighted, v) + dot_nn(q, p_ref[h]) * begin
        inv = lax.rsqrt(jnp.mean(attended * attended, axis=1, keepdims=True) + epsilon)
        normed = attended * inv
        gain = gain_ref[:, cols]
        out_ref[:, cols] = (normed * gain).astype(BF16)
        g = g_ref[:, cols].astype(F32)
        term_ref[0, h : h + 1, :] = jnp.sum(g * normed, axis=0, keepdims=True)
        scaled = g * gain
        ga = (inv * (scaled - normed * jnp.mean(scaled * normed, axis=1, keepdims=True))).astype(BF16)
        ga_ref[:, cols] = ga
        qd = (q.astype(F32) * begin).astype(BF16)
        l_ref[h] = dot_tn(qd, ga).astype(BF16)


def backward_kernel(
    heads, size, q_ref, k_ref, v_ref, ga_ref, ld_ref, p_ref, s_ref,
    gq_ref, gk_ref, gv_ref,
):
    ld = ld_ref[0]
    rows, columns, causal = cumulative(ld)
    tokens = ld.shape[1]
    start = jnp.exp(columns)
    end = jnp.exp(columns[tokens - 1 :, :] - columns)
    for h in range(heads):
        cols = slice(h * size, (h + 1) * size)
        q, k, v, ga = q_ref[:, cols], k_ref[:, cols], v_ref[:, cols], ga_ref[:, cols]
        weight = jnp.exp(jnp.where(causal, columns[:, h : h + 1] - rows[h : h + 1, :], NEG))
        weighted = (dot_nt(q, k) * weight).astype(BF16)
        gw = (dot_nt(ga, v) * weight).astype(BF16)
        begin, finish = start[:, h : h + 1], end[:, h : h + 1]
        gq_ref[:, cols] = (dot_nn(gw, k) + begin * dot_nt(ga, p_ref[h])).astype(BF16)
        gk_ref[:, cols] = (dot_tn(gw, q) + finish * dot_nt(v, s_ref[h])).astype(BF16)
        gv_ref[:, cols] = (dot_tn(weighted, ga) + finish * dot_nn(k, s_ref[h])).astype(BF16)


def scan_kernel(count, group, chunks, reverse, with_gain, *refs):
    if with_gain:
        (l_ref, a_ref, t_ref, p_ref, sum_ref, got, given, decay, carry_in, carry_out,
         got_send, got_recv, dec_send, dec_recv, car_send, car_recv, ret_send, ret_recv,
         gain_got, gain_send, gain_recv) = refs
    else:
        (l_ref, a_ref, p_ref, got, given, decay, carry_in, carry_out,
         got_send, got_recv, dec_send, dec_recv, car_send, car_recv, ret_send, ret_recv) = refs
    me = lax.axis_index("seq")
    dp = lax.axis_index("dp")
    planes = count // group
    mine = lax.rem(me, group)
    plane = me // group
    owned = l_ref.shape[0] // group
    piece = owned // chunks

    def owned_rows(peer, chunk):
        return pl.ds(peer * owned + chunk * piece, piece)

    def give_local(offset, chunk):
        peer = lax.rem(mine + offset, group)
        return pltpu.make_async_remote_copy(
            src_ref=l_ref.at[owned_rows(peer, chunk)],
            dst_ref=got.at[mine, pl.ds(chunk * piece, piece)],
            send_sem=got_send.at[offset, chunk],
            recv_sem=got_recv.at[offset, chunk],
            device_id=(plane * group + peer, dp),
            device_id_type=MESH,
        )

    def take_local(offset, chunk):
        peer = lax.rem(mine + group - offset, group)
        return pltpu.make_async_remote_copy(
            src_ref=l_ref.at[owned_rows(mine, chunk)],
            dst_ref=got.at[peer, pl.ds(chunk * piece, piece)],
            send_sem=got_send.at[offset, chunk],
            recv_sem=got_recv.at[offset, chunk],
            device_id=(plane * group + peer, dp),
            device_id_type=MESH,
        )

    def give_decay(offset):
        peer = lax.rem(mine + offset, group)
        return pltpu.make_async_remote_copy(
            src_ref=a_ref.at[pl.ds(peer * owned, owned)],
            dst_ref=decay.at[mine],
            send_sem=dec_send.at[offset],
            recv_sem=dec_recv.at[offset],
            device_id=(plane * group + peer, dp),
            device_id_type=MESH,
        )

    def take_decay(offset):
        peer = lax.rem(mine + group - offset, group)
        return pltpu.make_async_remote_copy(
            src_ref=a_ref.at[pl.ds(mine * owned, owned)],
            dst_ref=decay.at[peer],
            send_sem=dec_send.at[offset],
            recv_sem=dec_recv.at[offset],
            device_id=(plane * group + peer, dp),
            device_id_type=MESH,
        )

    def give_back(offset, chunk):
        peer = lax.rem(mine + offset, group)
        return pltpu.make_async_remote_copy(
            src_ref=given.at[peer, pl.ds(chunk * piece, piece)],
            dst_ref=p_ref.at[owned_rows(mine, chunk)],
            send_sem=ret_send.at[offset, chunk],
            recv_sem=ret_recv.at[offset, chunk],
            device_id=(plane * group + peer, dp),
            device_id_type=MESH,
        )

    def take_back(offset, chunk):
        peer = lax.rem(mine + group - offset, group)
        return pltpu.make_async_remote_copy(
            src_ref=given.at[mine, pl.ds(chunk * piece, piece)],
            dst_ref=p_ref.at[owned_rows(peer, chunk)],
            send_sem=ret_send.at[offset, chunk],
            recv_sem=ret_recv.at[offset, chunk],
            device_id=(plane * group + peer, dp),
            device_id_type=MESH,
        )

    step = planes - 1 if reverse else 1

    def carry(chunk):
        target = lax.rem(plane + step, planes) * group + mine
        return pltpu.make_async_remote_copy(
            src_ref=carry_out.at[pl.ds(chunk * piece, piece)],
            dst_ref=carry_in.at[pl.ds(chunk * piece, piece)],
            send_sem=car_send.at[chunk],
            recv_sem=car_recv.at[chunk],
            device_id=(target, dp),
            device_id_type=MESH,
        )

    first = plane == (planes - 1 if reverse else 0)
    final = plane == (0 if reverse else planes - 1)
    order = list(range(group))[::-1] if reverse else list(range(group))

    for offset in range(1, group):
        give_decay(offset).start()
    for chunk in range(chunks):
        for offset in range(1, group):
            give_local(offset, chunk).start()
    if with_gain:
        rows = gain_got.shape[1]
        total = 2 * count
        flat = me * 2 + dp

        def send_gain(offset, unused):
            there = lax.rem(flat + offset, total)
            pltpu.make_async_remote_copy(
                src_ref=t_ref.at[pl.ds((there // 2) * l_ref.shape[0] // count, rows)],
                dst_ref=gain_got.at[offset - 1],
                send_sem=gain_send,
                recv_sem=gain_recv,
                device_id=(there // 2, lax.rem(there, 2)),
                device_id_type=MESH,
            ).start()
            return unused

        lax.fori_loop(1, total, send_gain, 0)
    got[mine] = l_ref[pl.ds(mine * owned, owned)]
    decay[mine] = a_ref[pl.ds(mine * owned, owned)]

    @pl.when(first)
    def _():
        carry_in[...] = jnp.zeros_like(carry_in)

    for offset in range(1, group):
        take_decay(offset).wait_recv()
    for chunk in range(chunks):
        for offset in range(1, group):
            take_local(offset, chunk).wait_recv()

        @pl.when(jnp.logical_not(first))
        def _():
            carry(chunk).wait_recv()

        def combine(h, unused):
            value = carry_in[h].astype(F32)
            for g in order:
                given[g, h] = value.astype(BF16)
                value = decay[g, pl.ds(h, 1)] * value + got[g, h].astype(F32)
            carry_out[h] = value.astype(BF16)
            return unused

        lax.fori_loop(chunk * piece, (chunk + 1) * piece, combine, 0)

        @pl.when(jnp.logical_not(final))
        def _():
            carry(chunk).start()

        for offset in range(1, group):
            give_back(offset, chunk).start()
        p_ref[owned_rows(mine, chunk)] = given[mine, pl.ds(chunk * piece, piece)]

    if with_gain:
        everything = pltpu.make_async_copy(gain_got, gain_got, gain_recv)
        everything.wait()
        pltpu.make_async_copy(gain_got, gain_got, gain_send).wait()
        sum_ref[...] = jnp.sum(gain_got[...], axis=0) + t_ref[pl.ds(me * l_ref.shape[0] // count, rows)]

    for chunk in range(chunks):
        for offset in range(1, group):
            take_back(offset, chunk).wait_recv()
    for offset in range(1, group):
        give_decay(offset).wait_send()
        for chunk in range(chunks):
            give_local(offset, chunk).wait_send()
            give_back(offset, chunk).wait_send()

    @pl.when(jnp.logical_not(final))
    def _():
        for chunk in range(chunks):
            carry(chunk).wait_send()


def scan_call(count, states, decays, reverse, terms=None):
    heads, size, _ = states.shape
    group = 1 << ((count.bit_length()) // 2)
    owned = heads // group
    chunks = min(owned, 4)
    vmem = pl.BlockSpec(memory_space=pltpu.VMEM)
    dma = pltpu.SemaphoreType.DMA
    out_shape = [jax.ShapeDtypeStruct(states.shape, BF16)]
    args = [states, decays]
    scratch = [
        pltpu.VMEM((group, owned, size, size), BF16),
        pltpu.VMEM((group, owned, size, size), BF16),
        pltpu.VMEM((group, owned, size), F32),
        pltpu.VMEM((owned, size, size), BF16),
        pltpu.VMEM((owned, size, size), BF16),
        dma((group, chunks)),
        dma((group, chunks)),
        dma((group,)),
        dma((group,)),
        dma((chunks,)),
        dma((chunks,)),
        dma((group, chunks)),
        dma((group, chunks)),
    ]
    if terms is not None:
        rows = max(1, heads // count)
        args.append(terms)
        out_shape.append(jax.ShapeDtypeStruct((rows, size), F32))
        scratch += [pltpu.VMEM((2 * count - 1, rows, size), F32), dma, dma]
    return pl.pallas_call(
        functools.partial(scan_kernel, count, group, chunks, reverse, terms is not None),
        out_shape=out_shape,
        in_specs=[vmem] * len(args),
        out_specs=[vmem] * len(out_shape),
        scratch_shapes=scratch,
        compiler_params=pltpu.CompilerParams(
            has_side_effects=True, vmem_limit_bytes=48 * 1024 * 1024
        ),
        name="suffix_scan" if reverse else "prefix_scan",
    )(*args)


def body(count, queries, key_vectors, value_vectors, out_grad, log_decay, norm_gain):
    _, tokens, features = queries.shape
    heads = log_decay.shape[1]
    size = features // heads
    q, k, v, g = (x.reshape(tokens, features) for x in (queries, key_vectors, value_vectors, out_grad))
    per = 4
    steps = heads // per
    ld = log_decay.reshape(steps, per, tokens)
    gain = norm_gain.reshape(1, features)
    wide = pl.BlockSpec((tokens, per * size), lambda i: (0, i))
    decay_spec = pl.BlockSpec((1, per, tokens), lambda i: (i, 0, 0))
    state_spec = pl.BlockSpec((per, size, size), lambda i: (i, 0, 0))
    row_spec = pl.BlockSpec((1, per, size), lambda i: (i, 0, 0))
    gain_spec = pl.BlockSpec((1, per * size), lambda i: (0, i))
    wide_shape = jax.ShapeDtypeStruct((tokens, features), BF16)
    state_shape = jax.ShapeDtypeStruct((heads, size, size), BF16)
    row_shape = jax.ShapeDtypeStruct((steps, per, size), F32)
    params = pltpu.CompilerParams(vmem_limit_bytes=48 * 1024 * 1024)

    local_state, decays = pl.pallas_call(
        functools.partial(local_kernel, per, size),
        grid=(steps,),
        in_specs=[wide, wide, decay_spec],
        out_specs=[state_spec, row_spec],
        out_shape=[state_shape, row_shape],
        compiler_params=params,
        name="local_states",
    )(k, v, ld)
    decays = decays.reshape(heads, size)
    (prior,) = scan_call(count, local_state, decays, False)
    output, grad_attended, later_local, terms = pl.pallas_call(
        functools.partial(forward_kernel, per, size),
        grid=(steps,),
        in_specs=[wide, wide, wide, wide, decay_spec, gain_spec, state_spec],
        out_specs=[wide, wide, state_spec, row_spec],
        out_shape=[wide_shape, wide_shape, state_shape, row_shape],
        compiler_params=params,
        name="forward",
    )(q, k, v, g, ld, gain, prior)
    later, gain_rows = scan_call(count, later_local, decays, True, terms.reshape(heads, size))
    grad_q, grad_k, grad_v = pl.pallas_call(
        functools.partial(backward_kernel, per, size),
        grid=(steps,),
        in_specs=[wide, wide, wide, wide, decay_spec, state_spec, state_spec],
        out_specs=[wide, wide, wide],
        out_shape=[wide_shape, wide_shape, wide_shape],
        compiler_params=params,
        name="backward",
    )(q, k, v, grad_attended, ld, prior, later)
    share = features // count
    flat_rows = gain_rows.reshape(-1)
    if flat_rows.shape[0] == share:
        grad_gain = flat_rows
    else:
        begin = lax.axis_index("seq") * share % size
        grad_gain = lax.dynamic_slice(flat_rows, (begin,), (share,))
    return tuple(x.reshape(queries.shape) for x in (output, grad_q, grad_k, grad_v)) + (grad_gain,)


def solution(mesh):
    wide = P("dp", "seq", None)
    return jax.shard_map(
        functools.partial(body, mesh.shape["seq"]),
        mesh=mesh,
        in_specs=(wide, wide, wide, wide, P("dp", None, "seq"), P()),
        out_specs=(wide, wide, wide, wide, P("seq")),
        check_vma=False,
    )
```

```python
import functools

import jax
import jax.numpy as jnp
from jax import lax
from jax.experimental import pallas as pl
from jax.experimental.pallas import tpu as pltpu
from jax.sharding import PartitionSpec as P

epsilon = 1e-06
F32 = jnp.float32
BF16 = jnp.bfloat16
MESH = pl.DeviceIdType.MESH
NEG = -1e30


def dot_nn(a, b):
    return lax.dot_general(a, b, (((1,), (0,)), ((), ())), preferred_element_type=F32)


def dot_nt(a, b):
    return lax.dot_general(a, b, (((1,), (1,)), ((), ())), preferred_element_type=F32)


def dot_tn(a, b):
    return lax.dot_general(a, b, (((0,), (0,)), ((), ())), preferred_element_type=F32)


def cumulative(ld):
    tokens = ld.shape[1]
    i = lax.broadcasted_iota(jnp.int32, (tokens, tokens), 0)
    j = lax.broadcasted_iota(jnp.int32, (tokens, tokens), 1)
    lower = (i >= j).astype(F32)
    exact = lax.Precision.HIGHEST
    rows = lax.dot_general(
        ld, lower, (((1,), (1,)), ((), ())), precision=exact, preferred_element_type=F32
    )
    columns = lax.dot_general(
        lower, ld, (((1,), (1,)), ((), ())), precision=exact, preferred_element_type=F32
    )
    return rows, columns, i >= j


def fused_kernel(
    count, group, chunks,
    q_hbm, k_hbm, v_hbm, g_hbm, ld_ref, gain_ref,
    out_ref, gq_ref, gk_ref, gv_ref, sum_ref,
    q_ref, k_ref, v_ref, g_ref, ga_ref, weighted_ref, weight_ref, inside_ref,
    pk_ref, pv_ref, col_ref, row_ref, start_ref, end_ref, decay_ref, decay_got, term_ref, gain_got,
    local, got, given, carry_in, carry_out, state,
    in_sem, dec_send, dec_recv, gain_send, gain_recv,
    got_send, got_recv, car_send, car_recv, ret_send, ret_recv,
):
    me = lax.axis_index("seq")
    dp = lax.axis_index("dp")
    planes = count // group
    mine = lax.rem(me, group)
    plane = me // group
    heads, tokens = ld_ref.shape
    size = q_ref.shape[1] // heads
    owned = heads // group
    piece = owned // chunks
    width = piece * size
    FORWARD, BACKWARD = 0, 1

    loads = [
        pltpu.make_async_copy(src, dst, in_sem.at[n])
        for n, (src, dst) in enumerate(
            ((k_hbm, k_ref), (v_hbm, v_ref), (q_hbm, q_ref), (g_hbm, g_ref))
        )
    ]
    for load in loads:
        load.start()

    rows, columns, causal = cumulative(ld_ref[...])
    last = columns[tokens - 1 :, :]
    start, end = jnp.exp(columns), jnp.exp(last - columns)
    decay_ref[...] = jnp.broadcast_to(jnp.exp(rows[:, tokens - 1 :]), (heads, size))
    for n in range(heads // piece):
        part = slice(n * piece, (n + 1) * piece)
        col_ref[n] = columns[:, part]
        start_ref[n] = start[:, part]
        end_ref[n] = end[:, part]
        row_ref[n] = rows[part, :]

    def to_device(src, dst, send, recv, target):
        return pltpu.make_async_remote_copy(
            src_ref=src, dst_ref=dst, send_sem=send, recv_sem=recv,
            device_id=(target, dp), device_id_type=MESH,
        )

    def ahead(offset):
        return lax.rem(mine + offset, group)

    def behind(offset):
        return lax.rem(mine + group - offset, group)

    def owned_rows(peer, chunk):
        return pl.ds(peer * owned + chunk * piece, piece)

    def chunk_rows(chunk):
        return pl.ds(chunk * piece, piece)

    def locals_of(way, offset, chunk, owner, slot, target):
        return to_device(
            local.at[way, owned_rows(owner, chunk)],
            got.at[way, slot, chunk_rows(chunk)],
            got_send.at[way, offset, chunk],
            got_recv.at[way, offset, chunk],
            plane * group + target,
        )

    def give_local(way, offset, chunk):
        return locals_of(way, offset, chunk, ahead(offset), mine, ahead(offset))

    def take_local(way, offset, chunk):
        return locals_of(way, offset, chunk, mine, behind(offset), behind(offset))

    def returns_of(way, offset, chunk, slot, owner, target):
        return to_device(
            given.at[way, slot, chunk_rows(chunk)],
            state.at[way, owned_rows(owner, chunk)],
            ret_send.at[way, offset, chunk],
            ret_recv.at[way, offset, chunk],
            plane * group + target,
        )

    def give_back(way, offset, chunk):
        return returns_of(way, offset, chunk, ahead(offset), mine, ahead(offset))

    def take_back(way, offset, chunk):
        return returns_of(way, offset, chunk, mine, behind(offset), behind(offset))

    def decays_of(offset, owner, slot, target):
        return to_device(
            decay_ref.at[pl.ds(owner * owned, owned)],
            decay_got.at[slot],
            dec_send.at[offset],
            dec_recv.at[offset],
            plane * group + target,
        )

    def carry(way, chunk):
        step = 1 if way == FORWARD else planes - 1
        return to_device(
            carry_out.at[way, chunk_rows(chunk)],
            carry_in.at[way, chunk_rows(chunk)],
            car_send.at[way, chunk],
            car_recv.at[way, chunk],
            lax.rem(plane + step, planes) * group + mine,
        )

    lowest, highest = plane == 0, plane == planes - 1
    first = (lowest, highest)
    final = (highest, lowest)

    def send_locals(way, chunk):
        for offset in range(1, group):
            give_local(way, offset, chunk).start()
        got[way, mine, chunk_rows(chunk)] = local[way, owned_rows(mine, chunk)]

    def combine_chunk(way, chunk):
        for offset in range(1, group):
            take_local(way, offset, chunk).wait_recv()

        @pl.when(jnp.logical_not(first[way]))
        def _():
            carry(way, chunk).wait_recv()

        order = list(range(group))
        if way == BACKWARD:
            order = order[::-1]
        for n in range(piece):
            h = chunk * piece + n
            value = carry_in[way, h].astype(F32)
            for g in order:
                given[way, g, h] = value.astype(BF16)
                value = decay_got[g, pl.ds(h, 1)] * value + got[way, g, h].astype(F32)
            carry_out[way, h] = value.astype(BF16)

        @pl.when(jnp.logical_not(final[way]))
        def _():
            carry(way, chunk).start()

        for offset in range(1, group):
            give_back(way, offset, chunk).start()
        state[way, owned_rows(mine, chunk)] = given[way, mine, chunk_rows(chunk)]

    def wait_states(way, chunk):
        for offset in range(1, group):
            take_back(way, offset, chunk).wait_recv()

    def each_head(chunk, act):
        both = 2 if group % 2 == 0 else 1

        def step(pair, unused):
            for half in range(both):
                owner = pair * both + half
                n = owner * chunks + chunk
                for h in range(piece):
                    head = owner * owned + chunk * piece + h
                    cols = pl.ds(pl.multiple_of(head * size, size), size)
                    act(head, cols, n, slice(h, h + 1))
            return unused

        lax.fori_loop(0, group // both, step, 0)

    def local_act(head, cols, n, h):
        kd = (k_ref[:, cols].astype(F32) * end_ref[n][:, h]).astype(BF16)
        local[FORWARD, head] = dot_tn(kd, v_ref[:, cols]).astype(BF16)

    def inside_act(head, cols, n, h):
        weight = jnp.exp(jnp.where(causal, col_ref[n][:, h] - row_ref[n][h, :], NEG))
        weighted = (dot_nt(q_ref[:, cols], k_ref[:, cols]) * weight).astype(BF16)
        weight_ref[head] = weight
        weighted_ref[head] = weighted
        inside_ref[:, cols] = dot_nn(weighted, v_ref[:, cols])

    def attend_act(head, cols, n, h):
        q = q_ref[:, cols]
        begin = start_ref[n][:, h]
        attended = inside_ref[:, cols] + dot_nn(q, state[FORWARD, head]) * begin
        inv = lax.rsqrt(jnp.mean(attended * attended, axis=1, keepdims=True) + epsilon)
        normed = attended * inv
        gain = gain_ref[:, cols]
        out_ref[:, cols] = (normed * gain).astype(BF16)
        g = g_ref[:, cols].astype(F32)
        term_ref[pl.ds(head, 1), :] = jnp.sum(g * normed, axis=0, keepdims=True)
        scaled = g * gain
        ga = (inv * (scaled - normed * jnp.mean(scaled * normed, axis=1, keepdims=True))).astype(BF16)
        ga_ref[:, cols] = ga
        qd = (q.astype(F32) * begin).astype(BF16)
        local[BACKWARD, head] = dot_tn(qd, ga).astype(BF16)

    def grad_act(head, cols, n, h):
        q, k, v, ga = q_ref[:, cols], k_ref[:, cols], v_ref[:, cols], ga_ref[:, cols]
        gw = (dot_nt(ga, v) * weight_ref[head]).astype(BF16)
        begin = start_ref[n][:, h]
        gq_ref[:, cols] = (dot_nn(gw, k) + begin * dot_nt(ga, state[FORWARD, head])).astype(BF16)
        pk_ref[:, cols] = dot_tn(gw, q)
        pv_ref[:, cols] = dot_tn(weighted_ref[head], ga)

    def finish_act(head, cols, n, h):
        finish = end_ref[n][:, h]
        later = state[BACKWARD, head]
        gk_ref[:, cols] = (pk_ref[:, cols] + finish * dot_nt(v_ref[:, cols], later)).astype(BF16)
        gv_ref[:, cols] = (pv_ref[:, cols] + finish * dot_nn(k_ref[:, cols], later)).astype(BF16)

    def over(low, high, act):
        def step(chunk, unused):
            act(chunk)
            return unused

        lax.fori_loop(low, high, step, 0)

    for offset in range(1, group):
        decays_of(offset, ahead(offset), mine, ahead(offset)).start()
    decay_got[mine] = decay_ref[pl.ds(mine * owned, owned)]

    @pl.when(lowest)
    def _():
        carry_in[FORWARD] = jnp.zeros(carry_in.shape[1:], BF16)

    @pl.when(highest)
    def _():
        carry_in[BACKWARD] = jnp.zeros(carry_in.shape[1:], BF16)

    loads[0].wait()
    loads[1].wait()

    def local_chunk(chunk):
        each_head(chunk, local_act)
        send_locals(FORWARD, chunk)

    over(0, chunks, local_chunk)
    loads[2].wait()
    for offset in range(1, group):
        decays_of(offset, mine, behind(offset), behind(offset)).wait_recv()

    before = plane * chunks // planes

    def prefix_step(j):
        low = jnp.where(j == 0, 0, jnp.minimum(before + j - 1, chunks))
        high = jnp.where(j == chunks, chunks, jnp.minimum(before + j, chunks))
        over(low, high, lambda chunk: each_head(chunk, inside_act))

        @pl.when(j < chunks)
        def _():
            combine_chunk(FORWARD, j)

    over(0, chunks + 1, prefix_step)
    loads[3].wait()

    def attend_chunk(chunk):
        wait_states(FORWARD, chunk)
        each_head(chunk, attend_act)
        send_locals(BACKWARD, chunk)

    ahead_of = jnp.where(highest, chunks - 1, chunks)
    from_top = planes - 1 - plane
    early = jnp.minimum(from_top * chunks // max(planes - 1, 1), chunks)

    def suffix_step(j):
        over(
            jnp.where(j == 0, 0, jnp.where(j == 1, ahead_of, chunks)),
            jnp.where(j == 0, ahead_of, chunks),
            attend_chunk,
        )
        low = jnp.where(j == 0, 0, jnp.minimum(early + jnp.maximum(j - 2, 0), chunks))
        high = jnp.where(j == chunks, chunks, jnp.minimum(early + jnp.maximum(j - 1, 0), chunks))
        over(low, high, lambda chunk: each_head(chunk, grad_act))

        @pl.when(j < chunks)
        def _():
            combine_chunk(BACKWARD, j)

    over(0, chunks + 1, suffix_step)

    share = gain_got.shape[1]
    total = 2 * count
    flat = me * 2 + dp

    def send_gain(offset, unused):
        there = lax.rem(flat + offset, total)
        pltpu.make_async_remote_copy(
            src_ref=term_ref.at[pl.ds((there // 2) * heads // count, share)],
            dst_ref=gain_got.at[offset - 1],
            send_sem=gain_send,
            recv_sem=gain_recv,
            device_id=(there // 2, lax.rem(there, 2)),
            device_id_type=MESH,
        ).start()
        return unused

    lax.fori_loop(1, total, send_gain, 0)

    def finish_chunk(chunk):
        wait_states(BACKWARD, chunk)
        each_head(chunk, finish_act)

    over(0, chunks, finish_chunk)

    pltpu.make_async_copy(gain_got, gain_got, gain_recv).wait()
    pltpu.make_async_copy(gain_got, gain_got, gain_send).wait()
    sum_ref[...] = jnp.sum(gain_got[...], axis=0) + term_ref[pl.ds(me * heads // count, share)]

    def drain(chunk):
        for way in (FORWARD, BACKWARD):
            for offset in range(1, group):
                give_local(way, offset, chunk).wait_send()
                give_back(way, offset, chunk).wait_send()

            @pl.when(jnp.logical_not(final[way]))
            def _():
                carry(way, chunk).wait_send()

    over(0, chunks, drain)
    for offset in range(1, group):
        decays_of(offset, ahead(offset), mine, ahead(offset)).wait_send()


def body(count, queries, key_vectors, value_vectors, out_grad, log_decay, norm_gain):
    _, tokens, features = queries.shape
    heads = log_decay.shape[1]
    size = features // heads
    group = 1 << (count.bit_length() // 2)
    owned = heads // group
    chunks = min(owned, 4)
    piece = owned // chunks
    share = max(1, heads // count)
    q, k, v, g = (x.reshape(tokens, features) for x in (queries, key_vectors, value_vectors, out_grad))
    vmem = pl.BlockSpec(memory_space=pltpu.VMEM)
    anywhere = pl.BlockSpec(memory_space=pl.ANY)
    dma = pltpu.SemaphoreType.DMA
    wide = (tokens, features)
    states = (2, owned, size, size)
    exchange = (2, group, owned, size, size)
    whole = jax.ShapeDtypeStruct(wide, BF16)
    output, grad_q, grad_k, grad_v, gain_rows = pl.pallas_call(
        functools.partial(fused_kernel, count, group, chunks),
        out_shape=[whole] * 4 + [jax.ShapeDtypeStruct((share, size), F32)],
        in_specs=[anywhere] * 4 + [vmem] * 2,
        out_specs=[vmem] * 5,
        scratch_shapes=[pltpu.VMEM(wide, BF16)] * 5
        + [
            pltpu.VMEM((heads, tokens, tokens), BF16),
            pltpu.VMEM((heads, tokens, tokens), F32),
            pltpu.VMEM(wide, F32),
            pltpu.VMEM(wide, F32),
            pltpu.VMEM(wide, F32),
            pltpu.VMEM((heads // piece, tokens, piece), F32),
            pltpu.VMEM((heads // piece, piece, tokens), F32),
            pltpu.VMEM((heads // piece, tokens, piece), F32),
            pltpu.VMEM((heads // piece, tokens, piece), F32),
            pltpu.VMEM((heads, size), F32),
            pltpu.VMEM((group, owned, size), F32),
            pltpu.VMEM((heads, size), F32),
            pltpu.VMEM((2 * count - 1, share, size), F32),
            pltpu.VMEM((2, heads, size, size), BF16),
            pltpu.VMEM(exchange, BF16),
            pltpu.VMEM(exchange, BF16),
            pltpu.VMEM(states, BF16),
            pltpu.VMEM(states, BF16),
            pltpu.VMEM((2, heads, size, size), BF16),
            dma((4,)),
            dma((group,)),
            dma((group,)),
            dma,
            dma,
            dma((2, group, chunks)),
            dma((2, group, chunks)),
            dma((2, chunks)),
            dma((2, chunks)),
            dma((2, group, chunks)),
            dma((2, group, chunks)),
        ],
        compiler_params=pltpu.CompilerParams(
            has_side_effects=True, vmem_limit_bytes=54 * 1024 * 1024
        ),
        name="fused",
    )(q, k, v, g, log_decay.reshape(heads, tokens), norm_gain.reshape(1, features))
    part = features // count
    flat_rows = gain_rows.reshape(-1)
    if flat_rows.shape[0] == part:
        grad_gain = flat_rows
    else:
        begin = lax.axis_index("seq") * part % size
        grad_gain = lax.dynamic_slice(flat_rows, (begin,), (part,))
    return tuple(x.reshape(queries.shape) for x in (output, grad_q, grad_k, grad_v)) + (grad_gain,)


def solution(mesh):
    wide = P("dp", "seq", None)
    return jax.shard_map(
        functools.partial(body, mesh.shape["seq"]),
        mesh=mesh,
        in_specs=(wide, wide, wide, wide, P("dp", None, "seq"), P()),
        out_specs=(wide, wide, wide, wide, P("seq")),
        check_vma=False,
    )
```

```python
import functools

import jax
import jax.numpy as jnp
from jax import lax
from jax.experimental import pallas as pl
from jax.experimental.pallas import tpu as pltpu
from jax.sharding import PartitionSpec as P

epsilon = 1e-06
F32 = jnp.float32
BF16 = jnp.bfloat16
MESH = pl.DeviceIdType.MESH
NEG = -1e30


def dot_nn(a, b):
    return lax.dot_general(a, b, (((1,), (0,)), ((), ())), preferred_element_type=F32)


def dot_nt(a, b):
    return lax.dot_general(a, b, (((1,), (1,)), ((), ())), preferred_element_type=F32)


def dot_tn(a, b):
    return lax.dot_general(a, b, (((0,), (0,)), ((), ())), preferred_element_type=F32)


def cumulative(ld):
    tokens = ld.shape[1]
    i = lax.broadcasted_iota(jnp.int32, (tokens, tokens), 0)
    j = lax.broadcasted_iota(jnp.int32, (tokens, tokens), 1)
    lower = (i >= j).astype(F32)
    exact = lax.Precision.HIGHEST
    rows = lax.dot_general(
        ld, lower, (((1,), (1,)), ((), ())), precision=exact, preferred_element_type=F32
    )
    columns = lax.dot_general(
        lower, ld, (((1,), (1,)), ((), ())), precision=exact, preferred_element_type=F32
    )
    return rows, columns, i >= j


def fused_kernel(
    count, group, chunks,
    q_hbm, k_hbm, v_hbm, g_hbm, ld_ref, gain_ref,
    out_ref, gq_ref, gk_ref, gv_ref, sum_ref,
    q_ref, k_ref, v_ref, g_ref, ga_ref, weighted_ref, weight_ref, inside_ref,
    pv_ref, col_ref, row_ref, start_ref, end_ref, decay_ref, decay_got, term_ref, gain_got,
    local, got, given, carry_in, carry_out, state,
    in_sem, dec_send, dec_recv, gain_send, gain_recv,
    got_send, got_recv, car_send, car_recv, ret_send, ret_recv,
):
    me = lax.axis_index("seq")
    dp = lax.axis_index("dp")
    planes = count // group
    mine = lax.rem(me, group)
    plane = me // group
    heads, tokens = ld_ref.shape
    size = q_ref.shape[1] // heads
    owned = heads // group
    piece = owned // chunks
    width = piece * size
    FORWARD, BACKWARD = 0, 1

    loads = [
        pltpu.make_async_copy(src, dst, in_sem.at[n])
        for n, (src, dst) in enumerate(
            ((k_hbm, k_ref), (v_hbm, v_ref), (q_hbm, q_ref), (g_hbm, g_ref))
        )
    ]
    for load in loads:
        load.start()

    rows, columns, causal = cumulative(ld_ref[...])
    last = columns[tokens - 1 :, :]
    start, end = jnp.exp(columns), jnp.exp(last - columns)
    decay_ref[...] = jnp.broadcast_to(jnp.exp(rows[:, tokens - 1 :]), (heads, size))
    for n in range(heads // piece):
        part = slice(n * piece, (n + 1) * piece)
        col_ref[n] = columns[:, part]
        start_ref[n] = start[:, part]
        end_ref[n] = end[:, part]
        row_ref[n] = rows[part, :]

    def to_device(src, dst, send, recv, target):
        return pltpu.make_async_remote_copy(
            src_ref=src, dst_ref=dst, send_sem=send, recv_sem=recv,
            device_id=(target, dp), device_id_type=MESH,
        )

    def ahead(offset):
        return lax.rem(mine + offset, group)

    def behind(offset):
        return lax.rem(mine + group - offset, group)

    def owned_rows(peer, chunk):
        return pl.ds(peer * owned + chunk * piece, piece)

    def chunk_rows(chunk):
        return pl.ds(chunk * piece, piece)

    def locals_of(way, offset, chunk, owner, slot, target):
        return to_device(
            local.at[way, owned_rows(owner, chunk)],
            got.at[way, slot, chunk_rows(chunk)],
            got_send.at[way, offset, chunk],
            got_recv.at[way, offset, chunk],
            plane * group + target,
        )

    def give_local(way, offset, chunk):
        return locals_of(way, offset, chunk, ahead(offset), mine, ahead(offset))

    def take_local(way, offset, chunk):
        return locals_of(way, offset, chunk, mine, behind(offset), behind(offset))

    def returns_of(way, offset, chunk, slot, owner, target):
        return to_device(
            given.at[way, slot, chunk_rows(chunk)],
            state.at[way, owned_rows(owner, chunk)],
            ret_send.at[way, offset, chunk],
            ret_recv.at[way, offset, chunk],
            plane * group + target,
        )

    def give_back(way, offset, chunk):
        return returns_of(way, offset, chunk, ahead(offset), mine, ahead(offset))

    def take_back(way, offset, chunk):
        return returns_of(way, offset, chunk, mine, behind(offset), behind(offset))

    def decays_of(offset, owner, slot, target):
        return to_device(
            decay_ref.at[pl.ds(owner * owned, owned)],
            decay_got.at[slot],
            dec_send.at[offset],
            dec_recv.at[offset],
            plane * group + target,
        )

    def carry(way, chunk):
        step = 1 if way == FORWARD else planes - 1
        return to_device(
            carry_out.at[way, chunk_rows(chunk)],
            carry_in.at[way, chunk_rows(chunk)],
            car_send.at[way, chunk],
            car_recv.at[way, chunk],
            lax.rem(plane + step, planes) * group + mine,
        )

    lowest, highest = plane == 0, plane == planes - 1
    first = (lowest, highest)
    final = (highest, lowest)

    def send_locals(way, chunk):
        for offset in range(1, group):
            give_local(way, offset, chunk).start()
        got[way, mine, chunk_rows(chunk)] = local[way, owned_rows(mine, chunk)]

    def combine_chunk(way, chunk):
        for offset in range(1, group):
            take_local(way, offset, chunk).wait_recv()

        @pl.when(jnp.logical_not(first[way]))
        def _():
            carry(way, chunk).wait_recv()

        order = list(range(group))
        if way == BACKWARD:
            order = order[::-1]
        for n in range(piece):
            h = chunk * piece + n
            value = carry_in[way, h].astype(F32)
            for g in order:
                given[way, g, h] = value.astype(BF16)
                value = decay_got[g, pl.ds(h, 1)] * value + got[way, g, h].astype(F32)
            carry_out[way, h] = value.astype(BF16)

        @pl.when(jnp.logical_not(final[way]))
        def _():
            carry(way, chunk).start()

        for offset in range(1, group):
            give_back(way, offset, chunk).start()
        state[way, owned_rows(mine, chunk)] = given[way, mine, chunk_rows(chunk)]

    def wait_states(way, chunk):
        for offset in range(1, group):
            take_back(way, offset, chunk).wait_recv()

    def each_head(chunk, act):
        both = min(group, max(1, 4 // piece))

        def step(pair, unused):
            for half in range(both):
                owner = pair * both + half
                n = owner * chunks + chunk
                for h in range(piece):
                    head = owner * owned + chunk * piece + h
                    cols = pl.ds(pl.multiple_of(head * size, size), size)
                    act(head, cols, n, slice(h, h + 1))
            return unused

        lax.fori_loop(0, group // both, step, 0)

    def local_act(head, cols, n, h):
        kd = (k_ref[:, cols].astype(F32) * end_ref[n][:, h]).astype(BF16)
        local[FORWARD, head] = dot_tn(kd, v_ref[:, cols]).astype(BF16)

    def inside_act(head, cols, n, h):
        weight = jnp.exp(jnp.where(causal, col_ref[n][:, h] - row_ref[n][h, :], NEG))
        weighted = (dot_nt(q_ref[:, cols], k_ref[:, cols]) * weight).astype(BF16)
        weight_ref[head] = weight
        weighted_ref[head] = weighted
        inside_ref[:, cols] = dot_nn(weighted, v_ref[:, cols])

    def attend_act(head, cols, n, h):
        q = q_ref[:, cols]
        begin = start_ref[n][:, h]
        attended = inside_ref[:, cols] + dot_nn(q, state[FORWARD, head]) * begin
        inv = lax.rsqrt(jnp.mean(attended * attended, axis=1, keepdims=True) + epsilon)
        normed = attended * inv
        gain = gain_ref[:, cols]
        out_ref[:, cols] = (normed * gain).astype(BF16)
        g = g_ref[:, cols].astype(F32)
        term_ref[pl.ds(head, 1), :] = jnp.sum(g * normed, axis=0, keepdims=True)
        scaled = g * gain
        ga = (inv * (scaled - normed * jnp.mean(scaled * normed, axis=1, keepdims=True))).astype(BF16)
        ga_ref[:, cols] = ga
        qd = (q.astype(F32) * begin).astype(BF16)
        local[BACKWARD, head] = dot_tn(qd, ga).astype(BF16)

    def grad_act(head, cols, n, h):
        q, k, v, ga = q_ref[:, cols], k_ref[:, cols], v_ref[:, cols], ga_ref[:, cols]
        gw = (dot_nt(ga, v) * weight_ref[head]).astype(BF16)
        begin = start_ref[n][:, h]
        gq_ref[:, cols] = (dot_nn(gw, k) + begin * dot_nt(ga, state[FORWARD, head])).astype(BF16)
        inside_ref[:, cols] = dot_tn(gw, q)
        pv_ref[:, cols] = dot_tn(weighted_ref[head], ga)

    def finish_act(head, cols, n, h):
        finish = end_ref[n][:, h]
        later = state[BACKWARD, head]
        gk_ref[:, cols] = (inside_ref[:, cols] + finish * dot_nt(v_ref[:, cols], later)).astype(BF16)
        gv_ref[:, cols] = (pv_ref[:, cols] + finish * dot_nn(k_ref[:, cols], later)).astype(BF16)

    def over(low, high, act):
        def step(chunk, unused):
            act(chunk)
            return unused

        lax.fori_loop(low, high, step, 0)

    for offset in range(1, group):
        decays_of(offset, ahead(offset), mine, ahead(offset)).start()
    decay_got[mine] = decay_ref[pl.ds(mine * owned, owned)]

    @pl.when(lowest)
    def _():
        carry_in[FORWARD] = jnp.zeros(carry_in.shape[1:], BF16)

    @pl.when(highest)
    def _():
        carry_in[BACKWARD] = jnp.zeros(carry_in.shape[1:], BF16)

    loads[0].wait()
    loads[1].wait()

    def local_chunk(chunk):
        each_head(chunk, local_act)
        send_locals(FORWARD, chunk)

    over(0, chunks, local_chunk)
    loads[2].wait()
    for offset in range(1, group):
        decays_of(offset, mine, behind(offset), behind(offset)).wait_recv()

    before = plane * chunks // planes

    def prefix_step(j):
        low = jnp.where(j == 0, 0, jnp.minimum(before + j - 1, chunks))
        high = jnp.where(j == chunks, chunks, jnp.minimum(before + j, chunks))
        over(low, high, lambda chunk: each_head(chunk, inside_act))

        @pl.when(j < chunks)
        def _():
            combine_chunk(FORWARD, j)

    over(0, chunks + 1, prefix_step)
    loads[3].wait()

    def attend_chunk(chunk):
        wait_states(FORWARD, chunk)
        each_head(chunk, attend_act)
        send_locals(BACKWARD, chunk)

    from_top = planes - 1 - plane
    lead = 3 + 2 * from_top
    early = jnp.minimum(from_top * chunks // max(planes - 1, 1), chunks)

    def suffix_step(j):
        over(
            jnp.where(j == 0, 0, jnp.minimum(j - 1 + lead, chunks)),
            jnp.minimum(j + lead, chunks),
            attend_chunk,
        )
        low = jnp.where(j == 0, 0, jnp.minimum(early + jnp.maximum(j - 2, 0), chunks))
        high = jnp.where(j == chunks, chunks, jnp.minimum(early + jnp.maximum(j - 1, 0), chunks))
        over(low, high, lambda chunk: each_head(chunk, grad_act))

        @pl.when(j < chunks)
        def _():
            combine_chunk(BACKWARD, j)

    over(0, chunks + 1, suffix_step)

    share = gain_got.shape[1]
    total = 2 * count
    flat = me * 2 + dp

    def send_gain(offset, unused):
        there = lax.rem(flat + offset, total)
        pltpu.make_async_remote_copy(
            src_ref=term_ref.at[pl.ds((there // 2) * heads // count, share)],
            dst_ref=gain_got.at[offset - 1],
            send_sem=gain_send,
            recv_sem=gain_recv,
            device_id=(there // 2, lax.rem(there, 2)),
            device_id_type=MESH,
        ).start()
        return unused

    lax.fori_loop(1, total, send_gain, 0)

    def finish_chunk(chunk):
        wait_states(BACKWARD, chunk)
        each_head(chunk, finish_act)

    over(0, chunks, finish_chunk)

    pltpu.make_async_copy(gain_got, gain_got, gain_recv).wait()
    pltpu.make_async_copy(gain_got, gain_got, gain_send).wait()
    sum_ref[...] = jnp.sum(gain_got[...], axis=0) + term_ref[pl.ds(me * heads // count, share)]

    def drain(chunk):
        for way in (FORWARD, BACKWARD):
            for offset in range(1, group):
                give_local(way, offset, chunk).wait_send()
                give_back(way, offset, chunk).wait_send()

            @pl.when(jnp.logical_not(final[way]))
            def _():
                carry(way, chunk).wait_send()

    over(0, chunks, drain)
    for offset in range(1, group):
        decays_of(offset, ahead(offset), mine, ahead(offset)).wait_send()


def body(count, queries, key_vectors, value_vectors, out_grad, log_decay, norm_gain):
    _, tokens, features = queries.shape
    heads = log_decay.shape[1]
    size = features // heads
    group = 1 << (count.bit_length() // 2)
    owned = heads // group
    chunks = min(owned, 8)
    piece = owned // chunks
    share = max(1, heads // count)
    q, k, v, g = (x.reshape(tokens, features) for x in (queries, key_vectors, value_vectors, out_grad))
    vmem = pl.BlockSpec(memory_space=pltpu.VMEM)
    anywhere = pl.BlockSpec(memory_space=pltpu.HBM)
    dma = pltpu.SemaphoreType.DMA
    wide = (tokens, features)
    states = (2, owned, size, size)
    exchange = (2, group, owned, size, size)
    whole = jax.ShapeDtypeStruct(wide, BF16)
    output, grad_q, grad_k, grad_v, gain_rows = pl.pallas_call(
        functools.partial(fused_kernel, count, group, chunks),
        out_shape=[whole] * 4 + [jax.ShapeDtypeStruct((share, size), F32)],
        in_specs=[anywhere] * 4 + [vmem] * 2,
        out_specs=[vmem] * 5,
        scratch_shapes=[pltpu.VMEM(wide, BF16)] * 5
        + [
            pltpu.VMEM((heads, tokens, tokens), BF16),
            pltpu.VMEM((heads, tokens, tokens), F32),
            pltpu.VMEM(wide, F32),
            pltpu.VMEM(wide, F32),
            pltpu.VMEM((heads // piece, tokens, piece), F32),
            pltpu.VMEM((heads // piece, piece, tokens), F32),
            pltpu.VMEM((heads // piece, tokens, piece), F32),
            pltpu.VMEM((heads // piece, tokens, piece), F32),
            pltpu.VMEM((heads, size), F32),
            pltpu.VMEM((group, owned, size), F32),
            pltpu.VMEM((heads, size), F32),
            pltpu.VMEM((2 * count - 1, share, size), F32),
            pltpu.VMEM((2, heads, size, size), BF16),
            pltpu.VMEM(exchange, BF16),
            pltpu.VMEM(exchange, BF16),
            pltpu.VMEM(states, BF16),
            pltpu.VMEM(states, BF16),
            pltpu.VMEM((2, heads, size, size), BF16),
            dma((4,)),
            dma((group,)),
            dma((group,)),
            dma,
            dma,
            dma((2, group, chunks)),
            dma((2, group, chunks)),
            dma((2, chunks)),
            dma((2, chunks)),
            dma((2, group, chunks)),
            dma((2, group, chunks)),
        ],
        compiler_params=pltpu.CompilerParams(
            has_side_effects=True, vmem_limit_bytes=47 * 1024 * 1024
        ),
        name="fused",
    )(q, k, v, g, log_decay.reshape(heads, tokens), norm_gain.reshape(1, features))
    part = features // count
    flat_rows = gain_rows.reshape(-1)
    if flat_rows.shape[0] == part:
        grad_gain = flat_rows
    else:
        begin = lax.axis_index("seq") * part % size
        grad_gain = lax.dynamic_slice(flat_rows, (begin,), (part,))
    return tuple(x.reshape(queries.shape) for x in (output, grad_q, grad_k, grad_v)) + (grad_gain,)


def solution(mesh):
    wide = P("dp", "seq", None)
    return jax.shard_map(
        functools.partial(body, mesh.shape["seq"]),
        mesh=mesh,
        in_specs=(wide, wide, wide, wide, P("dp", None, "seq"), P()),
        out_specs=(wide, wide, wide, wide, P("seq")),
        check_vma=False,
    )
```
